16 devices in a mesh: ep: 16 (over z, y, x, core).
Axes of the slice: x: 2, y: 2, z: 2, core: 2. Of those that a mesh axis runs over, the one named last changes fastest.
Arguments:
- table_in: float32 [262144, 300], P('ep')
- table_out: float32 [262144, 300], P('ep')
- centers: int32 [65536], P('ep')
- contexts: int32 [65536], P('ep')
- negatives: int32 [65536, 10], P('ep')
Outputs:
- output 1: float32 [], replicated
- output 2: float32 [262144, 300], P('ep')
- output 3: float32 [262144, 300], P('ep')
All inputs are finite; a program needn't handle non-finite values.
Results may differ from the reference program's by a relative error of at most 0.001.
Values sent between devices are 32-bit elements.
A program may use at most 1 GiB of HBM per device.

```python
import math
import jax
import jax.numpy as jnp
from jax import lax

GROUP = 16
ROWS_DEV = 16384
PAIRS_DEV = 4096
DIM = 300
NEG = 10

VOCAB = GROUP * ROWS_DEV
N_PAIRS = GROUP * PAIRS_DEV
N_LOOK = PAIRS_DEV * (NEG + 2)
SHARE = N_LOOK // GROUP
PAIR_BLOCK = min(PAIRS_DEV, 1024)
ROOT_ROWS = math.isqrt(ROWS_DEV)
LEARN_RATE = 0.5


def draw_words(dev_key):
    key_extra, key_top, key_perm, key_root, key_rest = jax.random.split(dev_key, 5)
    slot_ids = jnp.arange(GROUP)
    extra_count = jax.random.randint(key_extra, (GROUP,), 0, SHARE // 2 + 1, dtype=jnp.int32)
    top_owner = jax.random.randint(key_top, (), 0, GROUP, dtype=jnp.int32)
    extra_count = jnp.where(slot_ids == top_owner, SHARE // 2, extra_count)
    extra_count = jnp.where(slot_ids == (top_owner + 1) % GROUP, 0, extra_count)
    owner_count = SHARE + extra_count - jnp.roll(extra_count, -1)
    owner_bounds = jnp.cumsum(owner_count)
    owners = jnp.searchsorted(owner_bounds, jnp.arange(N_LOOK), side='right')
    owners = jax.random.permutation(key_perm, owners.astype(jnp.int32))
    root_part = jax.random.randint(key_root, (N_LOOK,), 0, ROOT_ROWS, dtype=jnp.int32)
    local_row = root_part * root_part + jax.random.randint(key_rest, (N_LOOK,), 0, 2 * root_part + 1, dtype=jnp.int32)
    word_ids = (owners + GROUP * local_row).astype(jnp.int32)
    return word_ids[:PAIRS_DEV], word_ids[PAIRS_DEV:2 * PAIRS_DEV], word_ids[2 * PAIRS_DEV:].reshape(PAIRS_DEV, NEG)


def setup_inputs(seed: int = 0) -> dict:
    seed_key = jax.random.key(seed)
    key_in, key_out, key_words = jax.random.split(seed_key, 3)
    unit_scale = DIM ** -0.25
    table_in = unit_scale * jax.random.normal(key_in, (VOCAB, DIM), jnp.float32)
    table_out = unit_scale * jax.random.normal(key_out, (VOCAB, DIM), jnp.float32)
    centers, contexts, negatives = jax.vmap(draw_words)(jax.random.split(key_words, GROUP))
    return {'table_in': table_in, 'table_out': table_out,
            'centers': centers.reshape(N_PAIRS), 'contexts': contexts.reshape(N_PAIRS),
            'negatives': negatives.reshape(N_PAIRS, NEG)}


def reference(table_in, table_out, centers, contexts, negatives):
    def row_of(word_ids):
        return (word_ids % GROUP) * ROWS_DEV + word_ids // GROUP

    n_blocks = N_PAIRS // PAIR_BLOCK
    blocks = (row_of(centers).reshape(n_blocks, PAIR_BLOCK),
              row_of(contexts).reshape(n_blocks, PAIR_BLOCK),
              row_of(negatives).reshape(n_blocks, PAIR_BLOCK, NEG))

    def block_step(acc_state, pair_block):
        grad_in, grad_out, loss_sum = acc_state
        cen_rows, ctx_rows, neg_rows = pair_block
        u_vec = table_in[cen_rows]
        ctx_vec = table_out[ctx_rows]
        neg_vec = table_out[neg_rows]
        pos_score = jnp.sum(u_vec * ctx_vec, axis=-1)
        neg_score = jnp.sum(u_vec[:, None, :] * neg_vec, axis=-1)
        loss_sum = loss_sum - jnp.sum(jax.nn.log_sigmoid(pos_score)) - jnp.sum(jax.nn.log_sigmoid(-neg_score))
        pos_coef = jax.nn.sigmoid(pos_score) - 1.0
        neg_coef = jax.nn.sigmoid(neg_score)
        grad_u = pos_coef[:, None] * ctx_vec + jnp.sum(neg_coef[:, :, None] * neg_vec, axis=1)
        grad_in = grad_in.at[cen_rows].add(grad_u)
        grad_out = grad_out.at[ctx_rows].add(pos_coef[:, None] * u_vec)
        grad_neg = (neg_coef[:, :, None] * u_vec[:, None, :]).reshape(PAIR_BLOCK * NEG, DIM)
        grad_out = grad_out.at[neg_rows.reshape(PAIR_BLOCK * NEG)].add(grad_neg)
        return (grad_in, grad_out, loss_sum), None

    start_state = (jnp.zeros((VOCAB, DIM), jnp.float32), jnp.zeros((VOCAB, DIM), jnp.float32),
                   jnp.zeros((), jnp.float32))
    final_state, _ = lax.scan(block_step, start_state, blocks)
    grad_in, grad_out, loss_sum = final_state
    return (loss_sum / N_PAIRS, table_in - LEARN_RATE * grad_in, table_out - LEARN_RATE * grad_out)
```

```python
import functools

import jax
import jax.numpy as jnp
from jax import lax
from jax.experimental import pallas as pl
from jax.experimental.pallas import tpu as pltpu
from jax.sharding import PartitionSpec as P

LEARN_RATE = 0.5
LANES = 128
ROUNDS = ((768, 768), (1536, 768), (1536, 768), (1024, 512))
EXTRA = (1024, 512)
GROUP = 16
PIECE = 256
VMEM_CAP = 62 * 1024 * 1024


def params():
    return pltpu.CompilerParams(vmem_limit_bytes=VMEM_CAP)


def cost(us):
    return pl.CostEstimate(flops=int(us * 1e8), bytes_accessed=int(us * 1e6), transcendentals=0)


def rows_of(x, n_slab):
    x = x.T
    pad = n_slab * LANES - x.shape[1]
    x = jnp.concatenate([x, jnp.zeros((x.shape[0], pad), jnp.float32)], axis=1)
    return [x[:, k * LANES:(k + 1) * LANES] for k in range(n_slab)]


def spread(src_ref, dst_ref, n_slab):
    cols = src_ref.shape[1]
    for c in range(0, cols, PIECE):
        for k, part in enumerate(rows_of(src_ref[:, c:c + PIECE], n_slab)):
            dst_ref[pl.ds(c * n_slab + k, PIECE, stride=n_slab), :] = part


def gather_back(src_ref, dst_ref, n_slab):
    width, cols = dst_ref.shape
    for c in range(0, cols, PIECE):
        x = [src_ref[pl.ds(c * n_slab + k, PIECE, stride=n_slab), :] for k in range(n_slab)]
        dst_ref[:, c:c + PIECE] = jnp.concatenate(x, axis=1).T[:width]


def to_rows(table_t):
    width, rows = table_t.shape
    n_slab = -(-width // LANES)
    cols = 1024
    return pl.pallas_call(
        lambda x_ref, o_ref: spread(x_ref, o_ref, n_slab),
        grid=(rows // cols,),
        in_specs=[pl.BlockSpec((width, cols), lambda i: (0, i))],
        out_specs=pl.BlockSpec((cols * n_slab, LANES), lambda i: (i, 0)),
        out_shape=jax.ShapeDtypeStruct((rows * n_slab, LANES), jnp.float32),
        compiler_params=params(), cost_estimate=cost(22), name="to_rows",
    )(table_t)


def from_rows(flat, width):
    n_slab = -(-width // LANES)
    rows = flat.shape[0] // n_slab
    cols = 1024
    return pl.pallas_call(
        lambda x_ref, o_ref: gather_back(x_ref, o_ref, n_slab),
        grid=(rows // cols,),
        in_specs=[pl.BlockSpec((cols * n_slab, LANES), lambda i: (i, 0))],
        out_specs=pl.BlockSpec((width, cols), lambda i: (0, i)),
        out_shape=jax.ShapeDtypeStruct((width, rows), jnp.float32),
        compiler_params=params(), cost_estimate=cost(22), name="from_rows",
    )(flat)


def u_gather_kernel(n_slab, row_mask, pay_ref, base_ref, table_ref, *rest):
    *outs, tab, rows, sem = rest
    cp = pltpu.make_async_copy(table_ref, tab, sem)
    cp.start()
    cp.wait()
    base = base_ref[0]
    for out in outs:
        size = out.shape[1]

        def one(g, carry, base=base):
            for k in range(8):
                i = g * 8 + k
                row = pay_ref[base + i] & row_mask
                rows[pl.ds(i * n_slab, n_slab), :] = tab[pl.ds(row, n_slab), :]
            return carry

        lax.fori_loop(0, size // 8, one, 0)
        gather_back(rows, out, n_slab)
        base = base + size


def u_gather(table_rows, pay, base, sizes, width, n_slab, row_mask):
    return pl.pallas_call(
        functools.partial(u_gather_kernel, n_slab, row_mask),
        grid_spec=pltpu.PrefetchScalarGridSpec(
            num_scalar_prefetch=2, grid=(1,),
            in_specs=[pl.BlockSpec(memory_space=pl.ANY)],
            out_specs=[pl.BlockSpec((width, s), lambda i, pay, base: (0, 0)) for s in sizes],
            scratch_shapes=[pltpu.VMEM(table_rows.shape, jnp.float32),
                            pltpu.VMEM((max(sizes) * n_slab, LANES), jnp.float32),
                            pltpu.SemaphoreType.DMA],
        ),
        out_shape=[jax.ShapeDtypeStruct((width, s), jnp.float32) for s in sizes],
        compiler_params=params(), cost_estimate=cost(40), name="u_gather",
    )(pay, base, table_rows)


def add_rows(pay_ref, base, n_own, g_ref, rows, tab, n_slab, row_mask):
    size = g_ref.shape[1]
    spread(g_ref, rows, n_slab)
    n_here = jnp.clip(n_own - base, 0, size)

    def one(g, carry):
        for k in range(8):
            i = g * 8 + k
            at = pl.ds(pay_ref[base + i] & row_mask, n_slab)
            tab[at, :] = tab[at, :] + rows[pl.ds(i * n_slab, n_slab), :]
        return carry

    lax.fori_loop(0, (n_here + 7) // 8, one, 0)


def u_update_kernel(n_slab, row_mask, n_g, final, pay_ref, base_ref, table_ref, *rest):
    grads, (out, tab, rows, sem) = rest[:n_g], rest[n_g:]
    step = pl.program_id(0)

    @pl.when(step == 0)
    def _():
        cp = pltpu.make_async_copy(table_ref, tab, sem)
        cp.start()
        cp.wait()
        base = base_ref[0]
        for g_ref in grads:
            add_rows(pay_ref, base, base_ref[1], g_ref, rows, tab, n_slab, row_mask)
            base = base + g_ref.shape[1]
        if not final:
            cp = pltpu.make_async_copy(tab, out, sem)
            cp.start()
            cp.wait()

    if final:
        @pl.when(step > 0)
        def _():
            n = out.shape[1] * n_slab
            gather_back(tab.at[pl.ds(pl.multiple_of((step - 1) * n, n), n), :], out, n_slab)


def u_update(table_rows, grads, pay, base, n_slab, row_mask, final_width=None):
    final = final_width is not None
    sizes = [g.shape[1] for g in grads]
    cols = 1024
    rows = table_rows.shape[0] // n_slab
    if final:
        out_spec = pl.BlockSpec((final_width, cols), lambda i, pay, base: (0, jnp.maximum(i - 1, 0)))
        out_shape = jax.ShapeDtypeStruct((final_width, rows), jnp.float32)
    else:
        out_spec = pl.BlockSpec(memory_space=pl.ANY)
        out_shape = jax.ShapeDtypeStruct(table_rows.shape, jnp.float32)
    return pl.pallas_call(
        functools.partial(u_update_kernel, n_slab, row_mask, len(grads), final),
        grid_spec=pltpu.PrefetchScalarGridSpec(
            num_scalar_prefetch=2, grid=(rows // cols + 1 if final else 1,),
            in_specs=[pl.BlockSpec(memory_space=pl.ANY)]
            + [pl.BlockSpec(g.shape, lambda i, pay, base: (0, 0)) for g in grads],
            out_specs=out_spec,
            scratch_shapes=[pltpu.VMEM(table_rows.shape, jnp.float32),
                            pltpu.VMEM((max(sizes) * n_slab, LANES), jnp.float32),
                            pltpu.SemaphoreType.DMA],
        ),
        out_shape=out_shape,
        compiler_params=params(), cost_estimate=cost(45), name="u_update",
    )(pay, base, table_rows, *grads)


def pair_kernel(n_slab, row_bits, pay_ref, start_ref, table_ref, acc_ref, u_ref,
                p_ref, acc_out, loss_ref, tab, acc, urow, prow, prod, coef, bits, sems):
    step = pl.program_id(0)
    row_mask = (1 << row_bits) - 1

    @pl.when(step == 0)
    def _():
        cp0 = pltpu.make_async_copy(table_ref, tab, sems.at[0])
        cp1 = pltpu.make_async_copy(acc_ref, acc, sems.at[1])
        cp0.start()
        cp1.start()
        loss_ref[...] = jnp.zeros_like(loss_ref)
        cp0.wait()
        cp1.wait()

    spread(u_ref, urow, n_slab)
    prow[...] = jnp.zeros_like(prow)
    first = start_ref[step]
    last = start_ref[step + 1]
    lane_k = lax.broadcasted_iota(jnp.int32, (GROUP, LANES), 0)

    def places(i):
        pay = pay_ref[i]
        return pay, pl.ds(pay & row_mask, n_slab), pl.ds(pay >> (row_bits + 1), n_slab)

    def group(gi, carry):
        base = first + gi * GROUP
        for k in range(GROUP):
            pay, row, slot = places(base + k)
            bits[k:k + 1, :] = jnp.full((1, LANES), pay, jnp.int32)
            prod[k * n_slab:(k + 1) * n_slab, :] = tab[row, :] * urow[slot, :]
        total = prod[pl.ds(0, GROUP, stride=n_slab), :]
        for k in range(1, n_slab):
            total = total + prod[pl.ds(k, GROUP, stride=n_slab), :]
        score = jnp.sum(total, axis=1, keepdims=True)
        sg = jnp.where(((bits[...] >> row_bits) & 1) == 1, -1.0, 1.0)
        sg = jnp.where(lane_k < last - base, sg, 0.0)
        x = score * sg
        e = jnp.exp(-jnp.abs(x))
        loss_ref[...] += jnp.where(sg == 0.0, 0.0, jnp.maximum(x, 0.0) + jnp.log1p(e))
        sig = jnp.where(x >= 0, 1.0, e) / (1.0 + e)
        coef[...] = (-LEARN_RATE) * sg * sig
        for k in range(GROUP):
            _, row, slot = places(base + k)
            gk = coef[k:k + 1, :]
            acc[row, :] = acc[row, :] + gk * urow[slot, :]
            prow[slot, :] = prow[slot, :] + gk * tab[row, :]
        return carry

    lax.fori_loop(0, (last - first + GROUP - 1) // GROUP, group, 0)
    gather_back(prow, p_ref, n_slab)

    @pl.when(step == pl.num_programs(0) - 1)
    def _():
        cp = pltpu.make_async_copy(acc, acc_out, sems.at[0])
        cp.start()
        cp.wait()


def pair_step(table_rows, acc_rows, u_all, pay, starts, block, n_dev, n_slab, row_bits):
    width = u_all.shape[0] // n_dev
    nb = u_all.shape[1] // block
    blk = pl.BlockSpec((width, block), lambda i, pay, starts: (i // nb, i % nb))
    any_spec = pl.BlockSpec(memory_space=pl.ANY)
    return pl.pallas_call(
        functools.partial(pair_kernel, n_slab, row_bits),
        grid_spec=pltpu.PrefetchScalarGridSpec(
            num_scalar_prefetch=2,
            grid=(n_dev * nb,),
            in_specs=[any_spec, any_spec, blk],
            out_specs=[blk, any_spec, pl.BlockSpec((GROUP, LANES), lambda i, pay, starts: (0, 0))],
            scratch_shapes=[pltpu.VMEM(table_rows.shape, jnp.float32),
                            pltpu.VMEM(table_rows.shape, jnp.float32),
                            pltpu.VMEM((block * n_slab, LANES), jnp.float32),
                            pltpu.VMEM((block * n_slab, LANES), jnp.float32),
                            pltpu.VMEM((GROUP * n_slab, LANES), jnp.float32),
                            pltpu.VMEM((GROUP, LANES), jnp.float32),
                            pltpu.VMEM((GROUP, LANES), jnp.int32),
                            pltpu.SemaphoreType.DMA((2,))],
        ),
        out_shape=[jax.ShapeDtypeStruct(u_all.shape, jnp.float32),
                   jax.ShapeDtypeStruct(table_rows.shape, jnp.float32),
                   jax.ShapeDtypeStruct((GROUP, LANES), jnp.float32)],
        compiler_params=params(), cost_estimate=cost(u_all.shape[1] // 8), name="pair_step",
    )(pay, starts, table_rows, acc_rows, u_all)


def solution(mesh):
    group_size = mesh.shape['ep']

    def device_step(table_in, table_out, centers, contexts, negatives):
        rows_dev, width = table_in.shape
        n_pairs, n_neg = negatives.shape
        n_look = n_pairs * (n_neg + 2)
        capacity = (3 * n_look) // (2 * group_size)
        n_slab = -(-width // LANES)
        width8 = -(-width // 8) * 8
        dev_row_bits = (rows_dev - 1).bit_length()
        row_bits = (rows_dev * n_slab - 1).bit_length()
        row_mask = (1 << row_bits) - 1
        pair_bits = (n_pairs - 1).bit_length()
        me = lax.axis_index('ep')
        devs = jnp.arange(group_size, dtype=jnp.int32)

        c_owner = centers % group_size
        one_hot = (c_owner[:, None] == devs[None, :]).astype(jnp.float32)
        tri = jnp.tril(jnp.ones((LANES, LANES), jnp.float32))
        n_sub = n_pairs // LANES
        inner = jnp.einsum('ij,bjc->bic', tri, one_hot.reshape(n_sub, LANES, group_size),
                           precision=lax.Precision.HIGHEST)
        sub_tot = inner[:, -1, :]
        before = jnp.einsum('ij,jc->ic', jnp.tril(jnp.ones((n_sub, n_sub), jnp.float32), -1), sub_tot,
                            precision=lax.Precision.HIGHEST)
        cum = (inner + before[:, None, :]).reshape(n_pairs, group_size)
        local_rank = (jnp.sum(cum * one_hot, axis=1) - 0.5).astype(jnp.int32)
        counts = (jnp.sum(sub_tot, axis=0) + 0.5).astype(jnp.int32)

        place = (c_owner << pair_bits | local_rank) << (dev_row_bits + 1)
        top = jnp.int32(-2 ** 31)
        neg_t = negatives.T
        e_cen = top | place | (centers // group_size) << 1
        e_ctx = place | (contexts // group_size) << 1 | 1
        e_neg = place[None, :] | (neg_t // group_size) << 1
        entries = jnp.concatenate([e_cen, e_ctx, e_neg.reshape(n_pairs * n_neg)])
        owners = jnp.concatenate([c_owner, contexts % group_size, (neg_t % group_size).reshape(n_pairs * n_neg)])
        n_to = jnp.sum((owners[None, :] == devs[:, None]).astype(jnp.int32), axis=1)
        lack = jnp.cumsum(capacity - n_to)
        fill_ids = jnp.arange(capacity * group_size - n_look, dtype=jnp.int32)
        fill_owner = jnp.sum((fill_ids[None, :] >= lack[:, None]).astype(jnp.int32), axis=0)
        keys = jnp.concatenate([owners, fill_owner])
        words = jnp.concatenate([entries, jnp.full(fill_ids.shape, -1, jnp.int32)])
        _, words = lax.sort((keys, words), num_keys=1, is_stable=False)
        heads = jnp.broadcast_to(jnp.pad(counts, (0, LANES - group_size))[None, :], (group_size, LANES))
        sent = jnp.concatenate([words.reshape(group_size, capacity), heads], axis=1)
        got = lax.all_to_all(sent, 'ep', 0, 0)
        all_counts = got[:, capacity:capacity + group_size]
        got = got[:, :capacity]

        offs = jnp.cumsum(all_counts, axis=0) - all_counts
        totals = jnp.sum(all_counts, axis=0)
        owner_of = (got >> (dev_row_bits + 1 + pair_bits)) & (group_size - 1)
        rank = (got >> (dev_row_bits + 1)) & (n_pairs - 1)
        for c in range(group_size):
            rank = rank + jnp.where(owner_of == c, offs[:, c:c + 1], 0)
        n_all = n_pairs * group_size
        n_static = sum(size for size, _ in ROUNDS)
        base = n_static + (rank - n_static) // EXTRA[0] * EXTRA[0]
        size, block = EXTRA
        end = n_static
        for r_size, r_block in reversed(ROUNDS):
            inside = rank < end
            end -= r_size
            base = jnp.where(inside, end, base)
            size = jnp.where(inside, r_size, size)
            block = jnp.where(inside, r_block, block)
        in_round = rank - base
        key_v = n_all + group_size * base + owner_of * size + in_round
        key = jnp.where(got == -1, 2 ** 30, jnp.where(got < 0, rank, key_v))
        in_block = jnp.where(in_round >= block, in_round - block, in_round)
        pay = ((got >> 1) & (rows_dev - 1)) * n_slab | (got & 1) << row_bits
        pay = pay | (in_block * n_slab) << (row_bits + 1)
        key, pay = lax.sort((key.reshape(-1), pay.reshape(-1)), num_keys=1, is_stable=False)
        pay = jnp.concatenate([pay, jnp.zeros((LANES,), jnp.int32)])
        n_own = jnp.sum(jnp.where(devs == me, totals, 0))

        def starts_of(first, n_pair, n_block):
            n = group_size * n_pair // n_block
            bounds = n_all + group_size * first + jnp.arange(n + 1, dtype=jnp.int32) * n_block
            return jnp.sum((key[None, :] < bounds[:, None]).astype(jnp.int32), axis=1)

        u_rows = to_rows(table_in.T)
        o_rows = to_rows(table_out.T)
        zero = jnp.int32(0)
        us = u_gather(u_rows, pay, jnp.stack([zero]), [s for s, _ in ROUNDS], width8, n_slab, row_mask)
        acc, grads, loss, first = o_rows, [], jnp.float32(0.0), 0
        for (n_pair, n_block), u in zip(ROUNDS, us):
            u_all = lax.all_gather(u, 'ep', tiled=True)
            p_all, acc, part = pair_step(o_rows, acc, u_all, pay, starts_of(first, n_pair, n_block),
                                         n_block, group_size, n_slab, row_bits)
            grads.append(lax.psum_scatter(p_all, 'ep', scatter_dimension=0, tiled=True))
            loss = loss + jnp.sum(part[:, 0])
            first += n_pair
        new_rows = u_update(u_rows, grads[:-1], pay, jnp.stack([zero, n_own]), n_slab, row_mask)
        last_base = jnp.stack([jnp.int32(first - ROUNDS[-1][0]), n_own])
        new_u = u_update(new_rows, grads[-1:], pay, last_base, n_slab, row_mask, final_width=width)
        new_o = from_rows(acc, width)
        total = lax.psum(loss, 'ep')

        n_most = jnp.max(totals)

        def more(state):
            first, t_u, t_o, t_loss = state
            u, = u_gather(u_rows, pay, jnp.stack([first]), [EXTRA[0]], width8, n_slab, row_mask)
            u_all = lax.all_gather(u, 'ep', tiled=True)
            p_all, t_acc, part = pair_step(o_rows, to_rows(t_o), u_all, pay, starts_of(first, *EXTRA),
                                           EXTRA[1], group_size, n_slab, row_bits)
            grad = lax.psum_scatter(p_all, 'ep', scatter_dimension=0, tiled=True)
            t_u = u_update(to_rows(t_u), [grad], pay, jnp.stack([first, n_own]), n_slab, row_mask,
                           final_width=width)
            return first + EXTRA[0], t_u, from_rows(t_acc, width), t_loss + lax.psum(jnp.sum(part[:, 0]), 'ep')

        _, new_u, new_o, total = lax.while_loop(lambda s: s[0] < n_most, more,
                                                (jnp.int32(first), new_u, new_o, total))
        return total / n_all, new_u.T, new_o.T

    return jax.shard_map(device_step, mesh=mesh,
                         in_specs=(P('ep', None), P('ep', None), P('ep'), P('ep'), P('ep', None)),
                         out_specs=(P(), P('ep', None), P('ep', None)), check_vma=False)
```

```python
import functools

import jax
import jax.numpy as jnp
from jax import lax
from jax.experimental import pallas as pl
from jax.experimental.pallas import tpu as pltpu
from jax.sharding import PartitionSpec as P

LEARN_RATE = 0.5
LANES = 128
ROUNDS = ((768, 768), (1536, 768), (1536, 768), (1152, 384))
EXTRA = (768, 768)
BLOCK_MAX = max(block for _, block in ROUNDS + (EXTRA,))
GROUP = 24
PIECE = 128
VMEM_CAP = 62 * 1024 * 1024


def params():
    return pltpu.CompilerParams(vmem_limit_bytes=VMEM_CAP)


def cost(us):
    return pl.CostEstimate(flops=int(us * 1e8), bytes_accessed=int(us * 1e6), transcendentals=0)


def rows_of(x, n_slab):
    x = x.T
    pad = n_slab * LANES - x.shape[1]
    x = jnp.concatenate([x, jnp.zeros((x.shape[0], pad), jnp.float32)], axis=1)
    return [x[:, k * LANES:(k + 1) * LANES] for k in range(n_slab)]


def spread(src_ref, dst_ref, n_slab):
    cols = src_ref.shape[1]
    for c in range(0, cols, PIECE):
        for k, part in enumerate(rows_of(src_ref[:, c:c + PIECE], n_slab)):
            dst_ref[pl.ds(c * n_slab + k, PIECE, stride=n_slab), :] = part


def gather_back(src_ref, dst_ref, n_slab):
    width, cols = dst_ref.shape
    for c in range(0, cols, PIECE):
        x = [src_ref[pl.ds(c * n_slab + k, PIECE, stride=n_slab), :] for k in range(n_slab)]
        dst_ref[:, c:c + PIECE] = jnp.concatenate(x, axis=1).T[:width]


def to_rows(table_t):
    width, rows = table_t.shape
    n_slab = -(-width // LANES)
    cols = 1024
    return pl.pallas_call(
        lambda x_ref, o_ref: spread(x_ref, o_ref, n_slab),
        grid=(rows // cols,),
        in_specs=[pl.BlockSpec((width, cols), lambda i: (0, i))],
        out_specs=pl.BlockSpec((cols * n_slab, LANES), lambda i: (i, 0)),
        out_shape=jax.ShapeDtypeStruct((rows * n_slab, LANES), jnp.float32),
        compiler_params=params(), cost_estimate=cost(22), name="to_rows",
    )(table_t)


def from_rows(flat, width):
    n_slab = -(-width // LANES)
    rows = flat.shape[0] // n_slab
    cols = 1024
    return pl.pallas_call(
        lambda x_ref, o_ref: gather_back(x_ref, o_ref, n_slab),
        grid=(rows // cols,),
        in_specs=[pl.BlockSpec((cols * n_slab, LANES), lambda i: (i, 0))],
        out_specs=pl.BlockSpec((width, cols), lambda i: (0, i)),
        out_shape=jax.ShapeDtypeStruct((width, rows), jnp.float32),
        compiler_params=params(), cost_estimate=cost(22), name="from_rows",
    )(flat)


def u_gather_kernel(n_slab, row_mask, pay_ref, base_ref, table_ref, *rest):
    *outs, tab, rows, sem = rest
    cp = pltpu.make_async_copy(table_ref, tab, sem)
    cp.start()
    cp.wait()
    base = base_ref[0]
    for out in outs:
        size = out.shape[1]

        def one(g, carry, base=base):
            for k in range(8):
                i = g * 8 + k
                row = pay_ref[base + i]
                rows[pl.ds(i * n_slab, n_slab), :] = tab[pl.ds(row, n_slab), :]
            return carry

        lax.fori_loop(0, size // 8, one, 0)
        gather_back(rows, out, n_slab)
        base = base + size


def u_gather(table_rows, pay, base, sizes, width, n_slab, row_mask):
    return pl.pallas_call(
        functools.partial(u_gather_kernel, n_slab, row_mask),
        grid_spec=pltpu.PrefetchScalarGridSpec(
            num_scalar_prefetch=2, grid=(1,),
            in_specs=[pl.BlockSpec(memory_space=pl.ANY)],
            out_specs=[pl.BlockSpec((width, s), lambda i, pay, base: (0, 0)) for s in sizes],
            scratch_shapes=[pltpu.VMEM(table_rows.shape, jnp.float32),
                            pltpu.VMEM((max(sizes) * n_slab, LANES), jnp.float32),
                            pltpu.SemaphoreType.DMA],
        ),
        out_shape=[jax.ShapeDtypeStruct((width, s), jnp.float32) for s in sizes],
        compiler_params=params(), cost_estimate=cost(40), name="u_gather",
    )(pay, base, table_rows)


def add_rows(pay_ref, base, n_own, g_ref, rows, tab, n_slab, row_mask):
    size = g_ref.shape[1]
    spread(g_ref, rows, n_slab)
    n_here = jnp.clip(n_own - base, 0, size)

    def one(g, carry):
        for k in range(8):
            i = g * 8 + k
            at = pl.ds(pay_ref[base + i], n_slab)
            tab[at, :] = tab[at, :] + rows[pl.ds(i * n_slab, n_slab), :]
        return carry

    lax.fori_loop(0, (n_here + 7) // 8, one, 0)


def u_update_kernel(n_slab, row_mask, n_g, final, pay_ref, base_ref, table_ref, *rest):
    grads, (out, tab, rows, sem) = rest[:n_g], rest[n_g:]
    step = pl.program_id(0)

    @pl.when(step == 0)
    def _():
        cp = pltpu.make_async_copy(table_ref, tab, sem)
        cp.start()
        cp.wait()
        base = base_ref[0]
        for g_ref in grads:
            add_rows(pay_ref, base, base_ref[1], g_ref, rows, tab, n_slab, row_mask)
            base = base + g_ref.shape[1]
        if not final:
            cp = pltpu.make_async_copy(tab, out, sem)
            cp.start()
            cp.wait()

    if final:
        @pl.when(step > 0)
        def _():
            n = out.shape[1] * n_slab
            gather_back(tab.at[pl.ds(pl.multiple_of((step - 1) * n, n), n), :], out, n_slab)


def u_update(table_rows, grads, pay, base, n_slab, row_mask, final_width=None):
    final = final_width is not None
    sizes = [g.shape[1] for g in grads]
    cols = 1024
    rows = table_rows.shape[0] // n_slab
    if final:
        out_spec = pl.BlockSpec((final_width, cols), lambda i, pay, base: (0, jnp.maximum(i - 1, 0)))
        out_shape = jax.ShapeDtypeStruct((final_width, rows), jnp.float32)
    else:
        out_spec = pl.BlockSpec(memory_space=pl.ANY)
        out_shape = jax.ShapeDtypeStruct(table_rows.shape, jnp.float32)
    return pl.pallas_call(
        functools.partial(u_update_kernel, n_slab, row_mask, len(grads), final),
        grid_spec=pltpu.PrefetchScalarGridSpec(
            num_scalar_prefetch=2, grid=(rows // cols + 1 if final else 1,),
            in_specs=[pl.BlockSpec(memory_space=pl.ANY)]
            + [pl.BlockSpec(g.shape, lambda i, pay, base: (0, 0)) for g in grads],
            out_specs=out_spec,
            scratch_shapes=[pltpu.VMEM(table_rows.shape, jnp.float32),
                            pltpu.VMEM((max(sizes) * n_slab, LANES), jnp.float32),
                            pltpu.SemaphoreType.DMA],
        ),
        out_shape=out_shape,
        compiler_params=params(), cost_estimate=cost(45), name="u_update",
    )(pay, base, table_rows, *grads)


def pair_kernel(n_slab, row_bits, pay_ref, start_ref, table_ref, acc_ref, u_ref,
                p_ref, acc_out, loss_ref, tab, acc, urow, prow, u_now, v_now, coef, bits,
                same_slot, same_row1, same_row2, terms, sems):
    step = pl.program_id(0)
    row_mask = (1 << row_bits) - 1
    slot_shift = row_bits + 4

    @pl.when(step == 0)
    def _():
        cp0 = pltpu.make_async_copy(table_ref, tab, sems.at[0])
        cp1 = pltpu.make_async_copy(acc_ref, acc, sems.at[1])
        cp0.start()
        cp1.start()
        loss_ref[...] = jnp.zeros_like(loss_ref)
        cp0.wait()
        cp1.wait()

    spread(u_ref, urow, n_slab)
    prow[...] = jnp.zeros_like(prow)
    first = start_ref[step]
    last = start_ref[step + 1]
    lane_k = lax.broadcasted_iota(jnp.int32, (GROUP, LANES), 0)

    def places(i):
        pay = pay_ref[i]
        return pay, pl.ds(pay & row_mask, n_slab), lax.shift_right_logical(pay, slot_shift)

    def scores(base, half, n_valid):
        top = half * GROUP * n_slab
        for k in range(GROUP):
            pay, row, slot = places(base + k)
            bits[k:k + 1, :] = jnp.full((1, LANES), pay, jnp.int32)
            v_now[top + k * n_slab:top + (k + 1) * n_slab, :] = tab[row, :]
            u_now[top + k * n_slab:top + (k + 1) * n_slab, :] = urow[pl.ds(slot, n_slab), :]
        total = jnp.zeros((GROUP, LANES), jnp.float32)
        for k in range(n_slab):
            at = pl.ds(top + k, GROUP, stride=n_slab)
            total = total + v_now[at, :] * u_now[at, :]
        score = jnp.sum(total, axis=1, keepdims=True)
        word = bits[...]
        sg = jnp.where(((word >> row_bits) & 1) == 1, -1.0, 1.0)
        if n_valid is not None:
            sg = jnp.where(lane_k < n_valid, sg, 0.0)
        x = score * sg
        e = jnp.exp(-jnp.abs(x))
        term = jnp.maximum(x, 0.0) + jnp.log1p(e)
        sig = jnp.where(x >= 0, 1.0, e) / (1.0 + e)
        at = pl.ds(half * GROUP, GROUP)
        terms[at, :] = term if n_valid is None else jnp.where(sg == 0.0, 0.0, term)
        coef[at, :] = (-LEARN_RATE) * sg * sig
        for j, ref in enumerate((same_slot, same_row1, same_row2)):
            ref[at, :] = ((word >> (row_bits + 1 + j)) & 1).astype(jnp.float32)

    def apply(base, half, run, n_valid):
        top = half * GROUP
        loss_ref[...] += terms[top:top + GROUP, :]
        for k in range(0, GROUP, 3):
            deltas, news, rows = [], [], []
            for j in range(k, min(k + 3, GROUP)):
                _, row, slot = places(base + j)
                if n_valid is not None:
                    slot = jnp.where(j < n_valid, slot, BLOCK_MAX * n_slab)
                h = top + j
                gj = coef[h:h + 1, :]
                at = slice(h * n_slab, (h + 1) * n_slab)
                delta = gj * u_now[at, :]
                new = acc[row, :] + delta
                if j > k:
                    new = new + same_row1[h:h + 1, :] * deltas[-1]
                if j > k + 1:
                    new = new + same_row2[h:h + 1, :] * deltas[-2]
                deltas.append(delta)
                news.append(new)
                rows.append(row)
                run = same_slot[h:h + 1, :] * run + gj * v_now[at, :]
                prow[pl.ds(slot, n_slab), :] = run
            for row, new in zip(rows, news):
                acc[row, :] = new
        return run

    def two_groups(gi, run):
        base = first + gi * (2 * GROUP)
        scores(base + GROUP, 1, None)
        run = apply(base, 0, run, None)
        scores(base + 2 * GROUP, 0, None)
        return apply(base + GROUP, 1, run, None)

    def tail_group(gi, run):
        base = tail + gi * GROUP
        n_valid = last - base
        scores(base, 0, n_valid)
        return apply(base, 0, run, n_valid)

    scores(first, 0, None)
    n_two = (last - first) // (2 * GROUP)
    run = lax.fori_loop(0, n_two, two_groups, jnp.zeros((n_slab, LANES), jnp.float32))
    tail = first + n_two * (2 * GROUP)
    lax.fori_loop(0, (last - tail + GROUP - 1) // GROUP, tail_group, run)

    gather_back(prow, p_ref, n_slab)

    @pl.when(step == pl.num_programs(0) - 1)
    def _():
        cp = pltpu.make_async_copy(acc, acc_out, sems.at[0])
        cp.start()
        cp.wait()


def pair_step(table_rows, acc_rows, u_all, pay, starts, block, n_dev, n_slab, row_bits):
    width = u_all.shape[0] // n_dev
    nb = u_all.shape[1] // block
    blk = pl.BlockSpec((width, block), lambda i, pay, starts: (i // nb, i % nb))
    any_spec = pl.BlockSpec(memory_space=pl.ANY)
    return pl.pallas_call(
        functools.partial(pair_kernel, n_slab, row_bits),
        grid_spec=pltpu.PrefetchScalarGridSpec(
            num_scalar_prefetch=2,
            grid=(n_dev * nb,),
            in_specs=[any_spec, any_spec, blk],
            out_specs=[blk, any_spec, pl.BlockSpec((GROUP, LANES), lambda i, pay, starts: (0, 0))],
            scratch_shapes=[pltpu.VMEM(table_rows.shape, jnp.float32),
                            pltpu.VMEM(table_rows.shape, jnp.float32),
                            pltpu.VMEM((BLOCK_MAX * n_slab, LANES), jnp.float32),
                            pltpu.VMEM(((BLOCK_MAX + 8) * n_slab, LANES), jnp.float32),
                            pltpu.VMEM((2 * GROUP * n_slab, LANES), jnp.float32),
                            pltpu.VMEM((2 * GROUP * n_slab, LANES), jnp.float32),
                            pltpu.VMEM((2 * GROUP, LANES), jnp.float32),
                            pltpu.VMEM((GROUP, LANES), jnp.int32),
                            pltpu.VMEM((2 * GROUP, LANES), jnp.float32),
                            pltpu.VMEM((2 * GROUP, LANES), jnp.float32),
                            pltpu.VMEM((2 * GROUP, LANES), jnp.float32),
                            pltpu.VMEM((2 * GROUP, LANES), jnp.float32),
                            pltpu.SemaphoreType.DMA((2,))],
        ),
        out_shape=[jax.ShapeDtypeStruct(u_all.shape, jnp.float32),
                   jax.ShapeDtypeStruct(table_rows.shape, jnp.float32),
                   jax.ShapeDtypeStruct((GROUP, LANES), jnp.float32)],
        compiler_params=params(), cost_estimate=cost(u_all.shape[1] // 8), name="pair_step",
    )(pay, starts, table_rows, acc_rows, u_all)


def solution(mesh):
    group_size = mesh.shape['ep']

    def device_step(table_in, table_out, centers, contexts, negatives):
        rows_dev, width = table_in.shape
        n_pairs, n_neg = negatives.shape
        capacity = (3 * n_pairs * (n_neg + 2)) // (2 * group_size)
        n_slab = -(-width // LANES)
        width8 = -(-width // 8) * 8
        dev_row_bits = (rows_dev - 1).bit_length()
        row_bits = (rows_dev * n_slab - 1).bit_length()
        row_mask = (1 << row_bits) - 1
        pair_bits = (n_pairs - 1).bit_length()
        me = lax.axis_index('ep')
        devs = jnp.arange(group_size, dtype=jnp.int32)

        n_all = n_pairs * group_size
        centers_all = lax.all_gather(centers, 'ep', tiled=True)
        owners_all = centers_all % group_size
        pair_ids = jnp.arange(n_all, dtype=jnp.int32)
        assert n_all * rows_dev <= 2 ** 30
        cen_key = jnp.where(owners_all == me, pair_ids * rows_dev + centers_all // group_size, 2 ** 30)
        cen_rows = (lax.sort(cen_key, is_stable=False) & (rows_dev - 1)) * n_slab
        cen_rows = jnp.concatenate([cen_rows, jnp.zeros((EXTRA[0],), jnp.int32)])
        all_counts = jnp.sum((owners_all.reshape(group_size, 1, n_pairs) == devs[None, :, None]).astype(jnp.int32),
                             axis=2)
        totals = jnp.sum(all_counts, axis=0)
        n_own = jnp.sum(jnp.where(devs == me, totals, 0))
        n_most = jnp.max(totals)

        c_owner = centers % group_size
        one_hot = (c_owner[:, None] == devs[None, :]).astype(jnp.float32)
        tri = jnp.tril(jnp.ones((LANES, LANES), jnp.float32))
        n_sub = n_pairs // LANES
        inner = jnp.einsum('ij,bjc->bic', tri, one_hot.reshape(n_sub, LANES, group_size),
                           precision=lax.Precision.HIGHEST)
        before = jnp.einsum('ij,jc->ic', jnp.tril(jnp.ones((n_sub, n_sub), jnp.float32), -1), inner[:, -1, :],
                            precision=lax.Precision.HIGHEST)
        cum = (inner + before[:, None, :]).reshape(n_pairs, group_size)
        local_rank = (jnp.sum(cum * one_hot, axis=1) - 0.5).astype(jnp.int32)

        place = (c_owner << pair_bits | local_rank) << (dev_row_bits + 1)
        neg_t = negatives.T
        e_ctx = place | (contexts // group_size) << 1 | 1
        e_neg = place[None, :] | (neg_t // group_size) << 1
        entries = jnp.concatenate([e_ctx, e_neg.reshape(n_pairs * n_neg)])
        owners = jnp.concatenate([contexts % group_size, (neg_t % group_size).reshape(n_pairs * n_neg)])
        n_to = jnp.sum((owners[None, :] == devs[:, None]).astype(jnp.int32), axis=1)
        lack = jnp.cumsum(capacity - n_to)
        fill_ids = jnp.arange(capacity * group_size - n_pairs * (n_neg + 1), dtype=jnp.int32)
        fill_owner = jnp.sum((fill_ids[None, :] >= lack[:, None]).astype(jnp.int32), axis=0)
        keys = jnp.concatenate([owners, fill_owner])
        words = jnp.concatenate([entries, jnp.full(fill_ids.shape, -1, jnp.int32)])
        _, words = lax.sort((keys, words), num_keys=1, is_stable=False)
        got = lax.all_to_all(words.reshape(group_size, capacity), 'ep', 0, 0)

        offs = jnp.cumsum(all_counts, axis=0) - all_counts
        owner_of = (got >> (dev_row_bits + 1 + pair_bits)) & (group_size - 1)
        rank = (got >> (dev_row_bits + 1)) & (n_pairs - 1)
        for c in range(group_size):
            rank = rank + jnp.where(owner_of == c, offs[:, c:c + 1], 0)
        n_static = sum(size for size, _ in ROUNDS)
        base = n_static + (rank - n_static) // EXTRA[0] * EXTRA[0]
        size, block = EXTRA
        end = n_static
        for r_size, r_block in reversed(ROUNDS):
            inside = rank < end
            end -= r_size
            base = jnp.where(inside, end, base)
            size = jnp.where(inside, r_size, size)
            block = jnp.where(inside, r_block, block)
        in_round = rank - base
        key = jnp.where(got == -1, 2 ** 30, group_size * base + owner_of * size + in_round)
        in_block = in_round
        for _ in range(max(n // b for n, b in ROUNDS + (EXTRA,)) - 1):
            in_block = jnp.where(in_block >= block, in_block - block, in_block)
        pay = ((got >> 1) & (rows_dev - 1)) * n_slab | (got & 1) << row_bits
        pay = pay | (in_block * n_slab) << (row_bits + 4)
        key, pay = lax.sort((key.reshape(-1), pay.reshape(-1)), num_keys=1, is_stable=False)
        row3 = pay & row_mask
        before = [jnp.concatenate([jnp.full((d,), -1, jnp.int32), row3[:-d]]) for d in (1, 2)]
        key_before = jnp.concatenate([jnp.full((1,), -1, jnp.int32), key[:-1]])
        for j, same in enumerate((key == key_before, row3 == before[0], row3 == before[1])):
            pay = pay | same.astype(jnp.int32) << (row_bits + 1 + j)
        pay = jnp.concatenate([pay, jnp.zeros((LANES,), jnp.int32)])
        assert 3 * GROUP <= LANES and row_bits + 4 + (BLOCK_MAX * n_slab - 1).bit_length() <= 32

        def starts_of(first, n_pair, n_block):
            n = group_size * n_pair // n_block
            bounds = group_size * first + jnp.arange(n + 1, dtype=jnp.int32) * n_block
            return jnp.sum((key[None, :] < bounds[:, None]).astype(jnp.int32), axis=1)

        u_rows = to_rows(table_in.T)
        o_rows = to_rows(table_out.T)
        zero = jnp.int32(0)
        us = u_gather(u_rows, cen_rows, jnp.stack([zero]), [s for s, _ in ROUNDS], width8, n_slab, row_mask)
        acc, grads, loss, first = o_rows, [], jnp.float32(0.0), 0
        for (n_pair, n_block), u in zip(ROUNDS, us):
            u_all = lax.all_gather(u, 'ep', tiled=True)
            p_all, acc, part = pair_step(o_rows, acc, u_all, pay, starts_of(first, n_pair, n_block),
                                         n_block, group_size, n_slab, row_bits)
            grads.append(lax.psum_scatter(p_all, 'ep', scatter_dimension=0, tiled=True))
            loss = loss + jnp.sum(part[:, 0])
            first += n_pair
        new_rows = u_update(u_rows, grads[:-1], cen_rows, jnp.stack([zero, n_own]), n_slab, row_mask)
        last_base = jnp.stack([jnp.int32(first - ROUNDS[-1][0]), n_own])
        new_u = u_update(new_rows, grads[-1:], cen_rows, last_base, n_slab, row_mask, final_width=width)
        new_o = from_rows(acc, width)
        total = lax.psum(loss, 'ep')

        def more(state):
            first, t_u, t_o, t_loss = state
            u, = u_gather(u_rows, cen_rows, jnp.stack([first]), [EXTRA[0]], width8, n_slab, row_mask)
            u_all = lax.all_gather(u, 'ep', tiled=True)
            p_all, t_acc, part = pair_step(o_rows, to_rows(t_o), u_all, pay, starts_of(first, *EXTRA),
                                           EXTRA[1], group_size, n_slab, row_bits)
            grad = lax.psum_scatter(p_all, 'ep', scatter_dimension=0, tiled=True)
            t_u = u_update(to_rows(t_u), [grad], cen_rows, jnp.stack([first, n_own]), n_slab, row_mask,
                           final_width=width)
            return first + EXTRA[0], t_u, from_rows(t_acc, width), t_loss + lax.psum(jnp.sum(part[:, 0]), 'ep')

        _, new_u, new_o, total = lax.while_loop(lambda s: s[0] < n_most, more,
                                                (jnp.int32(first), new_u, new_o, total))
        return total / n_all, new_u.T, new_o.T

    return jax.shard_map(device_step, mesh=mesh,
                         in_specs=(P('ep', None), P('ep', None), P('ep'), P('ep'), P('ep', None)),
                         out_specs=(P(), P('ep', None), P('ep', None)), check_vma=False)
```

```python
import functools

import jax
import jax.numpy as jnp
from jax import lax
from jax.experimental import pallas as pl
from jax.experimental.pallas import tpu as pltpu
from jax.sharding import PartitionSpec as P

LEARN_RATE = 0.5
LANES = 128
ROUNDS = ((1920, 640), (3072, 768))
EXTRA = (768, 768)
BLOCK_MAX = max(block for _, block in ROUNDS + (EXTRA,))
GROUP = 24
PIECE = 128
VMEM_CAP = 62 * 1024 * 1024


def params():
    return pltpu.CompilerParams(vmem_limit_bytes=VMEM_CAP)


def cost(us):
    return pl.CostEstimate(flops=int(us * 1e8), bytes_accessed=int(us * 1e6), transcendentals=0)


def rows_of(x, n_slab):
    x = x.T
    pad = n_slab * LANES - x.shape[1]
    x = jnp.concatenate([x, jnp.zeros((x.shape[0], pad), jnp.float32)], axis=1)
    return [x[:, k * LANES:(k + 1) * LANES] for k in range(n_slab)]


def spread(src_ref, dst_ref, n_slab):
    cols = src_ref.shape[1]
    for c in range(0, cols, PIECE):
        for k, part in enumerate(rows_of(src_ref[:, c:c + PIECE], n_slab)):
            dst_ref[pl.ds(c * n_slab + k, PIECE, stride=n_slab), :] = part


def gather_back(src_ref, dst_ref, n_slab):
    width, cols = dst_ref.shape
    for c in range(0, cols, PIECE):
        x = [src_ref[pl.ds(c * n_slab + k, PIECE, stride=n_slab), :] for k in range(n_slab)]
        dst_ref[:, c:c + PIECE] = jnp.concatenate(x, axis=1).T[:width]


def to_rows(table_t):
    width, rows = table_t.shape
    n_slab = -(-width // LANES)
    cols = 1024
    return pl.pallas_call(
        lambda x_ref, o_ref: spread(x_ref, o_ref, n_slab),
        grid=(rows // cols,),
        in_specs=[pl.BlockSpec((width, cols), lambda i: (0, i))],
        out_specs=pl.BlockSpec((cols * n_slab, LANES), lambda i: (i, 0)),
        out_shape=jax.ShapeDtypeStruct((rows * n_slab, LANES), jnp.float32),
        compiler_params=params(), cost_estimate=cost(22), name="to_rows",
    )(table_t)


def from_rows(flat, width):
    n_slab = -(-width // LANES)
    rows = flat.shape[0] // n_slab
    cols = 1024
    return pl.pallas_call(
        lambda x_ref, o_ref: gather_back(x_ref, o_ref, n_slab),
        grid=(rows // cols,),
        in_specs=[pl.BlockSpec((cols * n_slab, LANES), lambda i: (i, 0))],
        out_specs=pl.BlockSpec((width, cols), lambda i: (0, i)),
        out_shape=jax.ShapeDtypeStruct((width, rows), jnp.float32),
        compiler_params=params(), cost_estimate=cost(22), name="from_rows",
    )(flat)


def u_gather_kernel(n_slab, pay_ref, base_ref, table_ref, *rest):
    *outs, tab, rows = rest
    step = pl.program_id(0)
    part = table_ref.shape[1] * n_slab
    spread(table_ref, tab.at[pl.ds(pl.multiple_of(step * part, part), part), :], n_slab)

    @pl.when(step == pl.num_programs(0) - 1)
    def _():
        base = base_ref[0]
        for out in outs:
            size = out.shape[1]

            def one(g, carry, base=base):
                for k in range(8):
                    i = g * 8 + k
                    row = pay_ref[base + i]
                    rows[pl.ds(i * n_slab, n_slab), :] = tab[pl.ds(row, n_slab), :]
                return carry

            lax.fori_loop(0, size // 8, one, 0)
            gather_back(rows, out, n_slab)
            base = base + size


def u_gather(table_t, pay, base, sizes, width8, n_slab):
    width, n_rows = table_t.shape
    cols = 1024
    return pl.pallas_call(
        functools.partial(u_gather_kernel, n_slab),
        grid_spec=pltpu.PrefetchScalarGridSpec(
            num_scalar_prefetch=2, grid=(n_rows // cols,),
            in_specs=[pl.BlockSpec((width, cols), lambda i, pay, base: (0, i))],
            out_specs=[pl.BlockSpec((width8, s), lambda i, pay, base: (0, 0)) for s in sizes],
            scratch_shapes=[pltpu.VMEM((n_rows * n_slab, LANES), jnp.float32),
                            pltpu.VMEM((max(sizes) * n_slab, LANES), jnp.float32)],
        ),
        out_shape=[jax.ShapeDtypeStruct((width8, s), jnp.float32) for s in sizes],
        compiler_params=params(), cost_estimate=cost(40), name="u_gather",
    )(pay, base, table_t)


def add_rows(pay_ref, base, n_own, g_ref, rows, tab, n_slab):
    size = g_ref.shape[1]
    spread(g_ref, rows, n_slab)
    n_here = jnp.clip(n_own - base, 0, size)

    def one(g, carry):
        for k in range(8):
            i = g * 8 + k
            at = pl.ds(pay_ref[base + i], n_slab)
            tab[at, :] = tab[at, :] + rows[pl.ds(i * n_slab, n_slab), :]
        return carry

    lax.fori_loop(0, (n_here + 7) // 8, one, 0)


def u_update_kernel(n_slab, n_g, pay_ref, base_ref, table_ref, *rest):
    grads, (out, tab, rows, sem) = rest[:n_g], rest[n_g:]
    step = pl.program_id(0)
    part = table_ref.shape[1] * n_slab
    spread(table_ref, tab.at[pl.ds(pl.multiple_of(step * part, part), part), :], n_slab)

    @pl.when(step == pl.num_programs(0) - 1)
    def _():
        base = base_ref[0]
        for g_ref in grads:
            add_rows(pay_ref, base, base_ref[1], g_ref, rows, tab, n_slab)
            base = base + g_ref.shape[1]
        cp = pltpu.make_async_copy(tab, out, sem)
        cp.start()
        cp.wait()


def u_update(table_t, grads, pay, base, n_slab):
    width, n_rows = table_t.shape
    cols = 1024
    sizes = [g.shape[1] for g in grads]
    return pl.pallas_call(
        functools.partial(u_update_kernel, n_slab, len(grads)),
        grid_spec=pltpu.PrefetchScalarGridSpec(
            num_scalar_prefetch=2, grid=(n_rows // cols,),
            in_specs=[pl.BlockSpec((width, cols), lambda i, pay, base: (0, i))]
            + [pl.BlockSpec(g.shape, lambda i, pay, base: (0, 0)) for g in grads],
            out_specs=pl.BlockSpec(memory_space=pl.ANY),
            scratch_shapes=[pltpu.VMEM((n_rows * n_slab, LANES), jnp.float32),
                            pltpu.VMEM((max(sizes) * n_slab, LANES), jnp.float32),
                            pltpu.SemaphoreType.DMA],
        ),
        out_shape=jax.ShapeDtypeStruct((n_rows * n_slab, LANES), jnp.float32),
        compiler_params=params(), cost_estimate=cost(45), name="u_update",
    )(pay, base, table_t, *grads)


def u_finish_kernel(n_slab, pay_ref, base_ref, table_ref, g_ref, out, tab, rows, sem):
    step = pl.program_id(0)

    @pl.when(step == 0)
    def _():
        cp = pltpu.make_async_copy(table_ref, tab, sem)
        cp.start()
        cp.wait()
        add_rows(pay_ref, base_ref[0], base_ref[1], g_ref, rows, tab, n_slab)

    @pl.when(step > 0)
    def _():
        n = out.shape[1] * n_slab
        gather_back(tab.at[pl.ds(pl.multiple_of((step - 1) * n, n), n), :], out, n_slab)


def u_finish(table_rows, grad, pay, base, n_slab, width):
    cols = 1024
    n_rows = table_rows.shape[0] // n_slab
    return pl.pallas_call(
        functools.partial(u_finish_kernel, n_slab),
        grid_spec=pltpu.PrefetchScalarGridSpec(
            num_scalar_prefetch=2, grid=(n_rows // cols + 1,),
            in_specs=[pl.BlockSpec(memory_space=pl.ANY),
                      pl.BlockSpec(grad.shape, lambda i, pay, base: (0, 0))],
            out_specs=pl.BlockSpec((width, cols), lambda i, pay, base: (0, jnp.maximum(i - 1, 0))),
            scratch_shapes=[pltpu.VMEM(table_rows.shape, jnp.float32),
                            pltpu.VMEM((grad.shape[1] * n_slab, LANES), jnp.float32),
                            pltpu.SemaphoreType.DMA],
        ),
        out_shape=jax.ShapeDtypeStruct((width, n_rows), jnp.float32),
        compiler_params=params(), cost_estimate=cost(30), name="u_finish",
    )(pay, base, table_rows, grad)


def pair_kernel(n_slab, row_bits, pay_ref, start_ref, table_ref, acc_ref, u_ref,
                p_ref, acc_out, loss_ref, tab, acc, urow, prow, u_now, v_now, coef, bits,
                same_slot, same_row1, same_row2, terms, sems):
    step = pl.program_id(0)
    row_mask = (1 << row_bits) - 1
    slot_shift = row_bits + 4

    @pl.when(step == 0)
    def _():
        cp0 = pltpu.make_async_copy(table_ref, tab, sems.at[0])
        cp1 = pltpu.make_async_copy(acc_ref, acc, sems.at[1])
        cp0.start()
        cp1.start()
        loss_ref[...] = jnp.zeros_like(loss_ref)
        cp0.wait()
        cp1.wait()

    spread(u_ref, urow, n_slab)
    prow[...] = jnp.zeros_like(prow)
    first = start_ref[step]
    last = start_ref[step + 1]
    lane_k = lax.broadcasted_iota(jnp.int32, (GROUP, LANES), 0)

    def places(i):
        pay = pay_ref[i]
        return pay, pl.ds(pay & row_mask, n_slab), lax.shift_right_logical(pay, slot_shift)

    def scores(base, half, n_valid):
        top = half * GROUP * n_slab
        for k in range(GROUP):
            pay, row, slot = places(base + k)
            bits[k:k + 1, :] = jnp.full((1, LANES), pay, jnp.int32)
            v_now[top + k * n_slab:top + (k + 1) * n_slab, :] = tab[row, :]
            u_now[top + k * n_slab:top + (k + 1) * n_slab, :] = urow[pl.ds(slot, n_slab), :]
        total = jnp.zeros((GROUP, LANES), jnp.float32)
        for k in range(n_slab):
            at = pl.ds(top + k, GROUP, stride=n_slab)
            total = total + v_now[at, :] * u_now[at, :]
        score = jnp.sum(total, axis=1, keepdims=True)
        word = bits[...]
        sg = jnp.where(((word >> row_bits) & 1) == 1, -1.0, 1.0)
        if n_valid is not None:
            sg = jnp.where(lane_k < n_valid, sg, 0.0)
        x = score * sg
        e = jnp.exp(-jnp.abs(x))
        term = jnp.maximum(x, 0.0) + jnp.log1p(e)
        sig = jnp.where(x >= 0, 1.0, e) / (1.0 + e)
        at = pl.ds(half * GROUP, GROUP)
        terms[at, :] = term if n_valid is None else jnp.where(sg == 0.0, 0.0, term)
        coef[at, :] = (-LEARN_RATE) * sg * sig
        for j, ref in enumerate((same_slot, same_row1, same_row2)):
            ref[at, :] = ((word >> (row_bits + 1 + j)) & 1).astype(jnp.float32)

    def apply(base, half, run, n_valid):
        top = half * GROUP
        loss_ref[...] += terms[top:top + GROUP, :]
        for k in range(0, GROUP, 3):
            deltas, news, rows = [], [], []
            for j in range(k, min(k + 3, GROUP)):
                _, row, slot = places(base + j)
                if n_valid is not None:
                    slot = jnp.where(j < n_valid, slot, BLOCK_MAX * n_slab)
                h = top + j
                gj = coef[h:h + 1, :]
                at = slice(h * n_slab, (h + 1) * n_slab)
                delta = gj * u_now[at, :]
                new = acc[row, :] + delta
                if j > k:
                    new = new + same_row1[h:h + 1, :] * deltas[-1]
                if j > k + 1:
                    new = new + same_row2[h:h + 1, :] * deltas[-2]
                deltas.append(delta)
                news.append(new)
                rows.append(row)
                run = same_slot[h:h + 1, :] * run + gj * v_now[at, :]
                prow[pl.ds(slot, n_slab), :] = run
            for row, new in zip(rows, news):
                acc[row, :] = new
        return run

    def two_groups(gi, run):
        base = first + gi * (2 * GROUP)
        scores(base + GROUP, 1, None)
        run = apply(base, 0, run, None)
        scores(base + 2 * GROUP, 0, None)
        return apply(base + GROUP, 1, run, None)

    def tail_group(gi, run):
        base = tail + gi * GROUP
        n_valid = last - base
        scores(base, 0, n_valid)
        return apply(base, 0, run, n_valid)

    scores(first, 0, None)
    n_two = (last - first) // (2 * GROUP)
    run = lax.fori_loop(0, n_two, two_groups, jnp.zeros((n_slab, LANES), jnp.float32))
    tail = first + n_two * (2 * GROUP)
    lax.fori_loop(0, (last - tail + GROUP - 1) // GROUP, tail_group, run)

    gather_back(prow, p_ref, n_slab)

    @pl.when(step == pl.num_programs(0) - 1)
    def _():
        cp = pltpu.make_async_copy(acc, acc_out, sems.at[0])
        cp.start()
        cp.wait()


def pair_step(table_rows, acc_rows, u_all, pay, starts, block, n_dev, n_slab, row_bits):
    width = u_all.shape[0] // n_dev
    nb = u_all.shape[1] // block
    blk = pl.BlockSpec((width, block), lambda i, pay, starts: (i // nb, i % nb))
    any_spec = pl.BlockSpec(memory_space=pl.ANY)
    return pl.pallas_call(
        functools.partial(pair_kernel, n_slab, row_bits),
        grid_spec=pltpu.PrefetchScalarGridSpec(
            num_scalar_prefetch=2,
            grid=(n_dev * nb,),
            in_specs=[any_spec, any_spec, blk],
            out_specs=[blk, any_spec, pl.BlockSpec((GROUP, LANES), lambda i, pay, starts: (0, 0))],
            scratch_shapes=[pltpu.VMEM(table_rows.shape, jnp.float32),
                            pltpu.VMEM(table_rows.shape, jnp.float32),
                            pltpu.VMEM((BLOCK_MAX * n_slab, LANES), jnp.float32),
                            pltpu.VMEM(((BLOCK_MAX + 8) * n_slab, LANES), jnp.float32),
                            pltpu.VMEM((2 * GROUP * n_slab, LANES), jnp.float32),
                            pltpu.VMEM((2 * GROUP * n_slab, LANES), jnp.float32),
                            pltpu.VMEM((2 * GROUP, LANES), jnp.float32),
                            pltpu.VMEM((GROUP, LANES), jnp.int32),
                            pltpu.VMEM((2 * GROUP, LANES), jnp.float32),
                            pltpu.VMEM((2 * GROUP, LANES), jnp.float32),
                            pltpu.VMEM((2 * GROUP, LANES), jnp.float32),
                            pltpu.VMEM((2 * GROUP, LANES), jnp.float32),
                            pltpu.SemaphoreType.DMA((2,))],
        ),
        out_shape=[jax.ShapeDtypeStruct(u_all.shape, jnp.float32),
                   jax.ShapeDtypeStruct(table_rows.shape, jnp.float32),
                   jax.ShapeDtypeStruct((GROUP, LANES), jnp.float32)],
        compiler_params=params(), cost_estimate=cost(u_all.shape[1] // 8), name="pair_step",
    )(pay, starts, table_rows, acc_rows, u_all)


def solution(mesh):
    group_size = mesh.shape['ep']

    def device_step(table_in, table_out, centers, contexts, negatives):
        rows_dev, width = table_in.shape
        n_pairs, n_neg = negatives.shape
        capacity = (3 * n_pairs * (n_neg + 2)) // (2 * group_size)
        n_slab = -(-width // LANES)
        width8 = -(-width // 8) * 8
        dev_row_bits = (rows_dev - 1).bit_length()
        row_bits = (rows_dev * n_slab - 1).bit_length()
        row_mask = (1 << row_bits) - 1
        pair_bits = (n_pairs - 1).bit_length()
        me = lax.axis_index('ep')
        devs = jnp.arange(group_size, dtype=jnp.int32)

        n_all = n_pairs * group_size
        centers_all = lax.all_gather(centers, 'ep', tiled=True)
        owners_all = centers_all % group_size
        pair_ids = jnp.arange(n_all, dtype=jnp.int32)
        assert n_all * rows_dev <= 2 ** 30
        cen_key = jnp.where(owners_all == me, pair_ids * rows_dev + centers_all // group_size, 2 ** 30)
        cen_rows = (lax.sort(cen_key, is_stable=False) & (rows_dev - 1)) * n_slab
        cen_rows = jnp.concatenate([cen_rows, jnp.zeros((EXTRA[0],), jnp.int32)])
        all_counts = jnp.sum((owners_all.reshape(group_size, 1, n_pairs) == devs[None, :, None]).astype(jnp.int32),
                             axis=2)
        totals = jnp.sum(all_counts, axis=0)
        n_own = jnp.sum(jnp.where(devs == me, totals, 0))
        n_most = jnp.max(totals)

        c_owner = centers % group_size
        one_hot = (c_owner[:, None] == devs[None, :]).astype(jnp.float32)
        tri = jnp.tril(jnp.ones((LANES, LANES), jnp.float32))
        n_sub = n_pairs // LANES
        inner = jnp.einsum('ij,bjc->bic', tri, one_hot.reshape(n_sub, LANES, group_size),
                           precision=lax.Precision.HIGHEST)
        before = jnp.einsum('ij,jc->ic', jnp.tril(jnp.ones((n_sub, n_sub), jnp.float32), -1), inner[:, -1, :],
                            precision=lax.Precision.HIGHEST)
        cum = (inner + before[:, None, :]).reshape(n_pairs, group_size)
        local_rank = (jnp.sum(cum * one_hot, axis=1) - 0.5).astype(jnp.int32)

        place = (c_owner << pair_bits | local_rank) << (dev_row_bits + 1)
        neg_t = negatives.T
        e_ctx = place | (contexts // group_size) << 1 | 1
        e_neg = place[None, :] | (neg_t // group_size) << 1
        entries = jnp.concatenate([e_ctx, e_neg.reshape(n_pairs * n_neg)])
        owners = jnp.concatenate([contexts % group_size, (neg_t % group_size).reshape(n_pairs * n_neg)])
        n_to = jnp.sum((owners[None, :] == devs[:, None]).astype(jnp.int32), axis=1)
        lack = jnp.cumsum(capacity - n_to)
        fill_ids = jnp.arange(capacity * group_size - n_pairs * (n_neg + 1), dtype=jnp.int32)
        fill_owner = jnp.sum((fill_ids[None, :] >= lack[:, None]).astype(jnp.int32), axis=0)
        keys = jnp.concatenate([owners, fill_owner])
        words = jnp.concatenate([entries, jnp.full(fill_ids.shape, -1, jnp.int32)])
        _, words = lax.sort((keys, words), num_keys=1, is_stable=False)
        got = lax.all_to_all(words.reshape(group_size, capacity), 'ep', 0, 0)

        offs = jnp.cumsum(all_counts, axis=0) - all_counts
        owner_of = (got >> (dev_row_bits + 1 + pair_bits)) & (group_size - 1)
        rank = (got >> (dev_row_bits + 1)) & (n_pairs - 1)
        for c in range(group_size):
            rank = rank + jnp.where(owner_of == c, offs[:, c:c + 1], 0)
        n_static = sum(size for size, _ in ROUNDS)
        base = n_static + (rank - n_static) // EXTRA[0] * EXTRA[0]
        size, block = EXTRA
        end = n_static
        for r_size, r_block in reversed(ROUNDS):
            inside = rank < end
            end -= r_size
            base = jnp.where(inside, end, base)
            size = jnp.where(inside, r_size, size)
            block = jnp.where(inside, r_block, block)
        in_round = rank - base
        key = jnp.where(got == -1, 2 ** 30, group_size * base + owner_of * size + in_round)
        in_block = in_round
        for _ in range(max(n // b for n, b in ROUNDS + (EXTRA,)) - 1):
            in_block = jnp.where(in_block >= block, in_block - block, in_block)
        pay = ((got >> 1) & (rows_dev - 1)) * n_slab | (got & 1) << row_bits
        pay = pay | (in_block * n_slab) << (row_bits + 4)
        key, pay = lax.sort((key.reshape(-1), pay.reshape(-1)), num_keys=1, is_stable=False)
        row3 = pay & row_mask
        before = [jnp.concatenate([jnp.full((d,), -1, jnp.int32), row3[:-d]]) for d in (1, 2)]
        key_before = jnp.concatenate([jnp.full((1,), -1, jnp.int32), key[:-1]])
        for j, same in enumerate((key == key_before, row3 == before[0], row3 == before[1])):
            pay = pay | same.astype(jnp.int32) << (row_bits + 1 + j)
        pay = jnp.concatenate([pay, jnp.zeros((LANES,), jnp.int32)])
        assert 3 * GROUP <= LANES and row_bits + 4 + (BLOCK_MAX * n_slab - 1).bit_length() <= 32

        def starts_of(first, n_pair, n_block):
            n = group_size * n_pair // n_block
            bounds = group_size * first + jnp.arange(n + 1, dtype=jnp.int32) * n_block
            return jnp.sum((key[None, :] < bounds[:, None]).astype(jnp.int32), axis=1)

        o_rows = to_rows(table_out.T)
        zero = jnp.int32(0)
        us = u_gather(table_in.T, cen_rows, jnp.stack([zero]), [s for s, _ in ROUNDS], width8, n_slab)
        acc, grads, loss, first = o_rows, [], jnp.float32(0.0), 0
        for (n_pair, n_block), u in zip(ROUNDS, us):
            u_all = lax.all_gather(u, 'ep', tiled=True)
            p_all, acc, part = pair_step(o_rows, acc, u_all, pay, starts_of(first, n_pair, n_block),
                                         n_block, group_size, n_slab, row_bits)
            grads.append(lax.psum_scatter(p_all, 'ep', scatter_dimension=0, tiled=True))
            loss = loss + jnp.sum(part[:, 0])
            first += n_pair
        new_rows = u_update(table_in.T, grads[:-1], cen_rows, jnp.stack([zero, n_own]), n_slab)
        last_base = jnp.stack([jnp.int32(first - ROUNDS[-1][0]), n_own])
        new_u = u_finish(new_rows, grads[-1], cen_rows, last_base, n_slab, width)
        new_o = from_rows(acc, width)
        total = lax.psum(loss, 'ep')

        def more(state):
            first, t_u, t_o, t_loss = state
            u, = u_gather(table_in.T, cen_rows, jnp.stack([first]), [EXTRA[0]], width8, n_slab)
            u_all = lax.all_gather(u, 'ep', tiled=True)
            p_all, t_acc, part = pair_step(o_rows, to_rows(t_o), u_all, pay, starts_of(first, *EXTRA),
                                           EXTRA[1], group_size, n_slab, row_bits)
            grad = lax.psum_scatter(p_all, 'ep', scatter_dimension=0, tiled=True)
            t_u = from_rows(u_update(t_u, [grad], cen_rows, jnp.stack([first, n_own]), n_slab), width)
            return first + EXTRA[0], t_u, from_rows(t_acc, width), t_loss + lax.psum(jnp.sum(part[:, 0]), 'ep')

        _, new_u, new_o, total = lax.while_loop(lambda s: s[0] < n_most, more,
                                                (jnp.int32(first), new_u, new_o, total))
        return total / n_all, new_u.T, new_o.T

    return jax.shard_map(device_step, mesh=mesh,
                         in_specs=(P('ep', None), P('ep', None), P('ep'), P('ep'), P('ep', None)),
                         out_specs=(P(), P('ep', None), P('ep', None)), check_vma=False)
```
